64 devices in a mesh: dp: 4 (over x, y), tp: 16 (over z, core).
Axes of the slice: x: 2, y: 2, z: 8, core: 2. Of those that a mesh axis runs over, the one named last changes fastest.
The devices are a block of a 4x4x8 slice.
Arguments:
- hidden: bfloat16 [16384, 512], P(('dp', 'tp')), parts along dimension 0
- w_two: bfloat16 [512, 512], replicated
- ln_scale: float32 [2, 512], replicated
- ln_shift: float32 [2, 512], replicated
- embed: bfloat16 [51200, 512], P('tp')
- targets: int32 [2, 16384], P(None, ('dp', 'tp')), parts along dimension 1
- loss_mask: int32 [2, 16384], P(None, ('dp', 'tp')), parts along dimension 1
Outputs:
- output 1: float32 [2, 16384], P(None, ('dp', 'tp')), parts along dimension 1
- output 2: float32 [4], P('dp'), parts along dimension 0
- output 3: bfloat16 [16384, 512], P(('dp', 'tp')), parts along dimension 0
- output 4: float32 [204800, 512], P(('dp', 'tp')), parts along dimension 0
- output 5: float32 [2048, 512], P('dp'), parts along dimension 0
- output 6: float32 [8, 512], P('dp'), parts along dimension 0
- output 7: float32 [8, 512], P('dp'), parts along dimension 0
There are 4 independent parts. The reference program is written for one: setup_inputs(seed, part) draws one part's arguments, and reference() takes and returns one part's arrays. A program takes and returns all parts, laid end to end along the dimension named above; an argument that names none is the same for every part.
All inputs are finite; a program needn't handle non-finite values.
Results may differ from the reference program's by a relative error of at most 0.001.
Values are sent between devices in bfloat16 or wider.
A program may use at most 768 MiB of HBM per device.

```python
import math
import jax
import jax.numpy as jnp
from jax import lax

TOKENS_DEV = 256
GROUP_SIZE = 16
D_MODEL = 512
VOCAB_SIZE = 50304
TABLE_ROWS = 51200

TOKENS = TOKENS_DEV * GROUP_SIZE
ROW_BLOCK = math.gcd(TOKENS, 128)
BLOCKS = TOKENS // ROW_BLOCK
LN_EPS = 1e-5


def setup_inputs(seed: int = 0, part: int = 0) -> dict:
    base = jax.random.key(seed)
    k_w, k_g, k_b, k_e = jax.random.split(base, 4)
    part_key = jax.random.fold_in(base, part)
    k_h, k_t, k_m, k_l = jax.random.split(part_key, 4)
    hidden = jax.random.normal(k_h, (TOKENS, D_MODEL), jnp.float32).astype(jnp.bfloat16)
    w_two = (jax.random.normal(k_w, (D_MODEL, D_MODEL), jnp.float32) * D_MODEL ** -0.5).astype(jnp.bfloat16)
    ln_scale = 1.0 + 0.3 * jax.random.normal(k_g, (2, D_MODEL), jnp.float32)
    ln_shift = 0.3 * jax.random.normal(k_b, (2, D_MODEL), jnp.float32)
    embed = (jax.random.normal(k_e, (TABLE_ROWS, D_MODEL), jnp.float32) * (2.5 * D_MODEL ** -0.5)).astype(jnp.bfloat16)
    targets = jax.random.randint(k_t, (2, TOKENS), 0, VOCAB_SIZE, jnp.int32)
    keep_len = jax.random.randint(k_l, (2, GROUP_SIZE, 1), TOKENS_DEV // 4, TOKENS_DEV + 1, jnp.int32)
    keep_draw = jax.random.randint(k_m, (2, GROUP_SIZE, TOKENS_DEV), 0, 8, jnp.int32)
    position = jnp.arange(TOKENS_DEV, dtype=jnp.int32)
    keep = (position < keep_len) & ((keep_draw != 0) | (position == 0))
    loss_mask = keep.astype(jnp.int32).reshape(2, TOKENS)
    return {'hidden': hidden, 'w_two': w_two, 'ln_scale': ln_scale, 'ln_shift': ln_shift,
            'embed': embed, 'targets': targets, 'loss_mask': loss_mask}


def layer_norm(values, gain, bias):
    mean_val = jnp.mean(values, axis=-1, keepdims=True)
    centered = values - mean_val
    variance = jnp.mean(centered * centered, axis=-1, keepdims=True)
    return centered * lax.rsqrt(variance + LN_EPS) * gain + bias


def reference(hidden, w_two, ln_scale, ln_shift, embed, targets, loss_mask):
    proj_out = jnp.dot(hidden, w_two, preferred_element_type=jnp.float32).astype(jnp.bfloat16)
    norm_input = jnp.stack([hidden.astype(jnp.float32), proj_out.astype(jnp.float32)])
    normed, ln_back = jax.vjp(jax.vmap(layer_norm), norm_input, ln_scale, ln_shift)
    x_both = normed.astype(jnp.bfloat16)
    mask_f = loss_mask.astype(jnp.float32)
    token_count = jnp.sum(mask_f, axis=1)
    weight = mask_f / token_count[:, None]
    x_blocks = jnp.swapaxes(x_both.reshape(2, BLOCKS, ROW_BLOCK, D_MODEL), 0, 1)
    t_blocks = jnp.swapaxes(targets.reshape(2, BLOCKS, ROW_BLOCK), 0, 1)
    w_blocks = jnp.swapaxes(weight.reshape(2, BLOCKS, ROW_BLOCK), 0, 1)
    col_ids = jnp.arange(TABLE_ROWS, dtype=jnp.int32)

    def block_step(d_embed, block):
        x_blk, t_blk, w_blk = block
        raw_rows = []
        dx_rows = []
        for head_idx in range(2):
            logits = jnp.dot(x_blk[head_idx], embed.T, preferred_element_type=jnp.float32)
            log_norm = jax.nn.logsumexp(logits, axis=-1)
            is_target = col_ids[None, :] == t_blk[head_idx][:, None]
            tgt_logit = jnp.sum(jnp.where(is_target, logits, 0.0), axis=-1)
            probs_val = jnp.exp(logits - log_norm[:, None])
            d_logits = ((probs_val - is_target.astype(jnp.float32)) * w_blk[head_idx][:, None]).astype(jnp.bfloat16)
            d_embed = d_embed + jnp.dot(d_logits.T, x_blk[head_idx], preferred_element_type=jnp.float32)
            dx_rows.append(jnp.dot(d_logits, embed, preferred_element_type=jnp.float32))
            raw_rows.append(log_norm - tgt_logit)
        return d_embed, (jnp.stack(raw_rows), jnp.stack(dx_rows))

    d_embed, (raw_loss, d_x) = lax.scan(block_step, jnp.zeros((TABLE_ROWS, D_MODEL), jnp.float32),
                                        (x_blocks, t_blocks, w_blocks))
    raw_loss = jnp.swapaxes(raw_loss, 0, 1).reshape(2, TOKENS)
    d_x = jnp.swapaxes(d_x, 0, 1).reshape(2, TOKENS, D_MODEL)
    token_loss = raw_loss * mask_f
    total_loss = jnp.sum(token_loss / token_count[:, None]).reshape(1)
    d_norm_in, d_ln_scale, d_ln_shift = ln_back(d_x)
    d_proj = d_norm_in[1].astype(jnp.bfloat16)
    d_hidden = (d_norm_in[0] + jnp.dot(d_proj, w_two.T, preferred_element_type=jnp.float32)).astype(jnp.bfloat16)
    d_w_two = jnp.dot(hidden.T, d_proj, preferred_element_type=jnp.float32)
    return token_loss, total_loss, d_hidden, d_embed, d_w_two, d_ln_scale, d_ln_shift
```

```python
import functools

import jax
import jax.numpy as jnp
from jax import lax
from jax.experimental import pallas as pl
from jax.experimental.pallas import tpu as pltpu
from jax.sharding import PartitionSpec as P

LN_EPS = 1e-5
F32 = jnp.float32
BF16 = jnp.bfloat16
MESH = pl.DeviceIdType.MESH
MASKED = 3.0e38


def dot_nn(a, b):
    return lax.dot_general(a, b, (((1,), (0,)), ((), ())), preferred_element_type=F32)


def dot_nt(a, b):
    return lax.dot_general(a, b, (((1,), (1,)), ((), ())), preferred_element_type=F32)


def norm_rows(val, gain, bias):
    cen = val - jnp.mean(val, axis=-1, keepdims=True)
    var = jnp.mean(cen * cen, axis=-1, keepdims=True)
    return (cen * lax.rsqrt(var + LN_EPS) * gain + bias).astype(BF16)


def kernel(n, chunk, h_ref, w_ref, gain_ref, bias_ref, gcol_ref, e_ref, meta_ref,
           loss_ref, total_ref, dh_ref, de_out, dw_ref, dln_ref,
           h_all, x_all, et, de, dz, meta_all, st_loc, st_rcv, nm_own, nm_all, part, sib, ring,
           at_own, g_own, g_rcv, dwt, sm_own, sm_rcv, xu,
           h_ss, h_rs, meta_ss, meta_rs, st_ss, st_rs, nm_ss, nm_rs, sib_ss, sib_rs, ring_ss, ring_rs,
           g_ss, g_rs, dwt_ss, dwt_rs, sm_ss, sm_rs, de_sem):
    tok, dim = h_ref.shape
    half = tok // 2
    rows = e_ref.shape[0]
    chips = n // 2
    far = chips // 2
    units = n
    me = lax.axis_index('tp')
    zc = me // 2
    kc = lax.rem(me, 2)
    wrap = lambda c: lax.rem(c + 2 * chips, chips)
    right = wrap(zc + 1) * 2 + kc
    left = wrap(zc - 1) * 2 + kc
    other = zc * 2 + 1 - kc
    peer = lambda i: lax.rem(me + i, n)

    def rcopy(src, dst, ss, rs, dev):
        return pltpu.make_async_remote_copy(src_ref=src, dst_ref=dst, send_sem=ss, recv_sem=rs,
                                            device_id={'tp': dev}, device_id_type=MESH)

    barrier = pltpu.get_barrier_semaphore()

    def hello(i, c):
        pl.semaphore_signal(barrier, inc=1, device_id={'tp': peer(i)}, device_id_type=MESH)
        return c
    lax.fori_loop(1, n, hello, 0)
    pl.semaphore_wait(barrier, n - 1)

    def hcopy(kind, chip, part_idx, core):
        owner = chip * 2 + core
        rng = pl.ds(part_idx * half, half)
        dev = (right, left, other)[kind]
        return rcopy(h_all.at[owner, rng], h_all.at[owner, rng], h_ss.at[kind, chip, part_idx],
                     h_rs.at[owner, part_idx], dev)

    def hown(kind, part_idx):
        rng = pl.ds(part_idx * half, half)
        dev = (right, left, other)[kind]
        return rcopy(h_ref.at[rng], h_all.at[me, rng], h_ss.at[kind, zc, part_idx], h_rs.at[me, part_idx], dev)

    for kind, p in ((0, 0), (1, 1), (0, 1), (1, 0), (2, 0), (2, 1)):
        hown(kind, p).start()

    def bcast(src, dst, ss, rs):
        def go(i, c):
            o = peer(i)
            rcopy(src, dst.at[me], ss.at[o], rs.at[me], o).start()
            return c
        lax.fori_loop(1, n, go, 0)

    def wait_recv(dst, ss, rs):
        def go(i, c):
            o = peer(i)
            rcopy(dst.at[o], dst.at[o], ss.at[o], rs.at[o], o).wait_recv()
            return c
        lax.fori_loop(1, n, go, 0)

    def wait_send(dst, ss, rs):
        def go(i, c):
            o = peer(i)
            rcopy(dst.at[o], dst.at[o], ss.at[o], rs.at[o], o).wait_send()
            return c
        lax.fori_loop(1, n, go, 0)

    bcast(meta_ref, meta_all, meta_ss, meta_rs)
    meta_all[me] = meta_ref[...]
    h_all[me] = h_ref[...]

    r_i = lax.broadcasted_iota(jnp.int32, (dim, dim), 0)
    c_i = lax.broadcasted_iota(jnp.int32, (dim, dim), 1)
    eye = jnp.where(r_i == c_i, 1.0, 0.0).astype(BF16)
    for r0 in range(0, rows, chunk):
        et[:, r0:r0 + chunk] = dot_nt(eye, e_ref[r0:r0 + chunk, :]).astype(BF16)
    h_own = h_ref[...]
    at_own[0] = dot_nt(eye, h_own)
    at_own[1] = dot_nt(eye, dot_nn(h_own, w_ref[...]).astype(BF16))

    def chip_block(i, c):
        j = (i + 1) // 2
        lo = wrap(zc - j)
        hi = wrap(zc + j)

        @pl.when(i == 0)
        def _():
            for p in range(2):
                hcopy(2, zc, p, 1 - kc).wait_recv()

        @pl.when((lax.rem(i, 2) == 1) & (j < far))
        def _():
            for p in range(2):
                hcopy(0, lo, p, kc).wait_recv()
                if p == 0:
                    hcopy(0, lo, p, kc).start()
                else:
                    @pl.when(j < far - 1)
                    def _():
                        hcopy(0, lo, p, kc).start()
                hcopy(2, lo, p, kc).start()
                q = 1 - p
                hcopy(1, hi, q, kc).wait_recv()
                if q == 1:
                    hcopy(1, hi, q, kc).start()
                else:
                    @pl.when(j < far - 1)
                    def _():
                        hcopy(1, hi, q, kc).start()
                hcopy(2, hi, q, kc).start()
            for p in range(2):
                hcopy(2, lo, p, 1 - kc).wait_recv()
                hcopy(2, hi, p, 1 - kc).wait_recv()

        @pl.when(j == far)
        def _():
            for p in range(2):
                hcopy(p, lo, p, kc).wait_recv()
                hcopy(2, lo, p, kc).start()
            for p in range(2):
                hcopy(2, lo, p, 1 - kc).wait_recv()

        chip = jnp.where(lax.rem(i, 2) == 1, lo, hi)
        w_two = w_ref[...]
        for q in range(2):
            h_val = h_all[2 * chip + q]
            x_all[0, 2 * chip + q] = norm_rows(h_val.astype(F32), gain_ref[0:1, :], bias_ref[0:1, :])
            a_two = dot_nn(h_val, w_two).astype(BF16).astype(F32)
            x_all[1, 2 * chip + q] = norm_rows(a_two, gain_ref[1:2, :], bias_ref[1:2, :])

        for h in range(2):
            x = x_all[h, pl.ds(2 * chip, 2)].reshape(2 * tok, dim)
            z = dot_nt(e_ref[0:chunk, :], x)
            m = s = None
            for r0 in range(0, rows, chunk):
                z_next = dot_nt(e_ref[r0 + chunk:r0 + 2 * chunk, :], x) if r0 + chunk < rows else None
                z3 = z.reshape(chunk // 8, 8, 2 * tok)
                cm = jnp.max(z3, axis=0)
                if m is None:
                    m = cm
                    s = jnp.sum(jnp.exp(z3 - m[None]), axis=0)
                else:
                    mn = jnp.maximum(m, cm)
                    s = s * jnp.exp(m - mn) + jnp.sum(jnp.exp(z3 - mn[None]), axis=0)
                    m = mn
                z = z_next
            m_all = jnp.max(m, axis=0, keepdims=True)
            s_all = jnp.sum(s * jnp.exp(m - m_all), axis=0, keepdims=True)
            for q in range(2):
                for p in range(2):
                    cut = slice((2 * q + p) * half, (2 * q + p + 1) * half)
                    st_loc[2 * chip + q, 2 * h + p:2 * h + p + 1, :] = m_all[:, cut]
                    st_loc[2 * chip + q, 4 + 2 * h + p:5 + 2 * h + p, :] = s_all[:, cut]
        for q in range(2):
            o = 2 * chip + q

            @pl.when(o != me)
            def _():
                rcopy(st_loc.at[o], st_rcv.at[me], st_ss.at[o], st_rs.at[me], o).start()
        return c
    lax.fori_loop(0, chips, chip_block, 0)

    wait_recv(meta_all, meta_ss, meta_rs)
    counts = jnp.sum(meta_all[:, 4:8, :], axis=0)
    n_tok = []
    for h in range(2):
        two = jnp.sum(counts[2 * h:2 * h + 2, :], axis=1, keepdims=True)
        n_tok += [jnp.sum(two, axis=0, keepdims=True)] * 2
    n_tok = jnp.concatenate(n_tok, axis=0)
    mask = meta_ref[4:8, :]
    weight = mask / n_tok
    st_rcv[me] = st_loc[me]
    wait_recv(st_rcv, st_ss, st_rs)
    st = st_rcv[...]
    st_m, st_s = st[:, 0:4, :], st[:, 4:8, :]
    m_tok = jnp.max(st_m, axis=0)
    s_tok = jnp.sum(st_s * jnp.exp(st_m - m_tok[None]), axis=0)
    lse = m_tok + jnp.log(s_tok)
    lse_w = jnp.where(mask > 0.0, lse - jnp.log(jnp.maximum(weight, 1e-30)), MASKED)
    nm_own[...] = jnp.concatenate([lse_w, weight], axis=0)
    nm_all[me] = nm_own[...]
    bcast(nm_own, nm_all, nm_ss, nm_rs)
    de[...] = jnp.zeros_like(de)
    wait_recv(nm_all, nm_ss, nm_rs)

    sub_i = lax.broadcasted_iota(jnp.int32, (8, half), 0)
    base_row = (me * rows).astype(F32)

    def pick(tile, row):
        return jnp.sum(jnp.where(sub_i == row, tile, 0.0), axis=0, keepdims=True)

    def sib_copy(u):
        return rcopy(part.at[lax.rem(u, 2), 1 - kc], sib.at[u], sib_ss.at[u], sib_rs.at[u], other)

    def ring_copy(u, d):
        return rcopy(sib.at[u, d], ring.at[u, d], ring_ss.at[u, d], ring_rs.at[u, d], (right, left)[d])

    def pass_on(u):
        step = u // 2
        sib_copy(u).wait_recv()
        for d in range(2):
            @pl.when(step > 0)
            def _():
                ring_copy(u - 2, d).wait_recv()
                sib[u, d] = sib[u, d] + part[lax.rem(u, 2), kc, d] + ring[u - 2, d]

            @pl.when(step == 0)
            def _():
                sib[u, d] = sib[u, d] + part[lax.rem(u, 2), kc, d]

            @pl.when(step < chips - 1)
            def _():
                ring_copy(u, d).start()

    def unit(u, c):
        h = 1 - lax.rem(u, 2)
        step = u // 2
        plus = wrap(zc - 1 - step)
        minus = wrap(zc + 1 + step)
        lse_p, w_p, t_p = [], [], []
        for q in range(2):
            for p, chip in ((0, plus), (1, minus)):
                o = 2 * chip + q
                at = 2 * q + p
                xu[at * half:(at + 1) * half, :] = x_all[h, o, p * half:(p + 1) * half, :]
                lse_p.append(pick(nm_all[o], 2 * h + p))
                w_p.append(pick(nm_all[o], 4 + 2 * h + p))
                t_p.append(pick(meta_all[o], 2 * h + p))
        lse_v = jnp.broadcast_to(jnp.concatenate(lse_p, axis=1), (8, 2 * tok))
        w_v = jnp.broadcast_to(jnp.concatenate(w_p, axis=1), (8, 2 * tok))
        row8 = lax.broadcasted_iota(jnp.int32, (8, 2 * tok), 0).astype(F32)
        t_v = jnp.broadcast_to(jnp.concatenate(t_p, axis=1), (8, 2 * tok)) - base_row - row8
        x = xu[...]
        tz = jnp.zeros((8, 2 * tok), F32)
        z = dot_nt(e_ref[0:chunk, :], x)
        for r0 in range(0, rows, chunk):
            z_next = dot_nt(e_ref[r0 + chunk:r0 + 2 * chunk, :], x) if r0 + chunk < rows else None
            for g in range(0, chunk, 16):
                pieces = []
                for b in range(2):
                    z8 = z[g + 8 * b:g + 8 * b + 8, :]
                    hit = t_v == float(r0 + g + 8 * b)
                    tz = tz + jnp.where(hit, z8, 0.0)
                    pieces.append(jnp.exp(z8 - lse_v) - jnp.where(hit, w_v, 0.0))
                dz[r0 + g:r0 + g + 16, :] = jnp.concatenate(pieces, axis=0).astype(BF16)
            de[r0:r0 + chunk, :] += dot_nn(dz[r0:r0 + chunk, :], x)
            z = z_next
        dxt = dot_nn(et[...], dz[...])

        @pl.when(u >= 2)
        def _():
            sib_copy(u - 2).wait_send()
        slot = lax.rem(u, 2)
        for q in range(2):
            for p in range(2):
                cut = slice((2 * q + p) * half, (2 * q + p + 1) * half)
                part[slot, q, p, 0:dim, :] = dxt[:, cut]
                part[slot, q, p, dim:dim + 8, :] = tz[:, cut]
        sib_copy(u).start()

        @pl.when(u >= 1)
        def _():
            pass_on(u - 1)
        return c
    lax.fori_loop(0, units, unit, 0)
    de_copy = pltpu.make_async_copy(de, de_out, de_sem)
    de_copy.start()
    pass_on(units - 1)

    loss_rows = []
    sums = []
    da_all = []
    for h in range(2):
        u = units - 1 - h
        g_col = gcol_ref[:, h:h + 1]
        acc_s = acc_b = None
        da_h = []
        for p in range(2):
            a = at_own[h, :, p * half:(p + 1) * half]
            cen = a - jnp.mean(a, axis=0, keepdims=True)
            rstd = lax.rsqrt(jnp.mean(cen * cen, axis=0, keepdims=True) + LN_EPS)
            xh = cen * rstd
            dx = sib[u, p, 0:dim, :]
            tgt = jnp.sum(sib[u, p, dim:dim + 8, :], axis=0, keepdims=True)
            loss_rows.append((lse[2 * h + p:2 * h + p + 1, :] - tgt) * mask[2 * h + p:2 * h + p + 1, :])
            dy = dx * g_col
            c1 = jnp.mean(dy, axis=0, keepdims=True)
            c2 = jnp.mean(dy * xh, axis=0, keepdims=True)
            da_h.append(rstd * (dy - c1 - xh * c2))
            acc_s = dx * xh if acc_s is None else acc_s + dx * xh
            acc_b = dx if acc_b is None else acc_b + dx
        da_all.append(jnp.concatenate(da_h, axis=1))
        sums.append((jnp.sum(acc_s.T, axis=0, keepdims=True), jnp.sum(acc_b.T, axis=0, keepdims=True)))
    loss = jnp.concatenate(loss_rows, axis=0)
    loss_ref[...] = loss
    frac = loss / n_tok
    loss_row = jnp.concatenate([frac[i:i + 1, :] for i in range(4)], axis=1)
    sm_own[...] = jnp.concatenate([sums[0][0], sums[1][0], sums[0][1], sums[1][1], loss_row,
                                   jnp.zeros((3, dim), F32)], axis=0)
    sm_rcv[me] = sm_own[...]
    bcast(sm_own, sm_rcv, sm_ss, sm_rs)
    d_proj = da_all[1].astype(BF16)
    width = dim // n
    for i in range(n):
        g_own[i] = d_proj[i * width:(i + 1) * width, :]
    g_rcv[me] = g_own[me]

    def g_send(i, c):
        o = peer(i)
        rcopy(g_own.at[o], g_rcv.at[me], g_ss.at[o], g_rs.at[me], o).start()
        return c
    lax.fori_loop(1, n, g_send, 0)
    dht = da_all[0] + dot_nn(w_ref[...], d_proj)
    dh_ref[...] = dht.T.astype(BF16)

    wait_recv(g_rcv, g_ss, g_rs)
    dw_slice = jnp.zeros((width, dim), F32)
    for o in range(n):
        dw_slice = dw_slice + dot_nn(g_rcv[o], h_all[o])
    dwt[me] = dw_slice

    def dw_send(i, c):
        o = peer(i)
        rcopy(dwt.at[me], dwt.at[me], dwt_ss.at[o], dwt_rs.at[me], o).start()
        return c
    lax.fori_loop(1, n, dw_send, 0)

    wait_recv(sm_rcv, sm_ss, sm_rs)
    sm = jnp.sum(sm_rcv[...], axis=0)
    dln_ref[...] = sm[0:4, :]
    total_ref[...] = jnp.broadcast_to(jnp.sum(sm[4:5, :], axis=1, keepdims=True), total_ref.shape)
    wait_recv(dwt, dwt_ss, dwt_rs)
    dw_ref[...] = dwt[...].reshape(dim, dim).T

    for ref, ss, rs in ((meta_all, meta_ss, meta_rs), (st_rcv, st_ss, st_rs), (nm_all, nm_ss, nm_rs),
                        (g_rcv, g_ss, g_rs), (dwt, dwt_ss, dwt_rs), (sm_rcv, sm_ss, sm_rs)):
        wait_send(ref, ss, rs)
    for kind in range(3):
        for p in range(2):
            hown(kind, p).wait_send()

    def h_done(j, c):
        lo = wrap(zc - j)
        hi = wrap(zc + j)
        hcopy(0, lo, 0, kc).wait_send()
        hcopy(1, hi, 1, kc).wait_send()

        @pl.when(j < far - 1)
        def _():
            hcopy(0, lo, 1, kc).wait_send()
            hcopy(1, hi, 0, kc).wait_send()
        for p in range(2):
            hcopy(2, lo, p, kc).wait_send()
            hcopy(2, hi, p, kc).wait_send()
        return c
    lax.fori_loop(1, far, h_done, 0)
    for p in range(2):
        hcopy(2, wrap(zc + far), p, kc).wait_send()
    for u in (units - 2, units - 1):
        sib_copy(u).wait_send()

    def ring_done(u, c):
        for d in range(2):
            ring_copy(u, d).wait_send()
        return c
    lax.fori_loop(0, units - 2, ring_done, 0)
    de_copy.wait()


def pick_chunk(rows):
    best = 128
    for c in range(128, min(rows, 640) + 1, 128):
        if rows % c == 0:
            best = c
    return best


def solution(mesh):
    n = mesh.shape['tp']
    tok_spec = P(('dp', 'tp'), None)
    row_spec = P(None, ('dp', 'tp'))

    def device_step(hidden, w_two, ln_scale, ln_shift, embed, targets, loss_mask):
        tok, dim = hidden.shape
        half = tok // 2
        rows = embed.shape[0]
        width = dim // n
        meta = jnp.concatenate([targets.reshape(4, half), loss_mask.reshape(4, half)], axis=0).astype(F32)
        vmem = pl.BlockSpec(memory_space=pltpu.VMEM)
        dma = pltpu.SemaphoreType.DMA
        outs = pl.pallas_call(
            functools.partial(kernel, n, pick_chunk(rows)),
            name='two_head_step',
            out_shape=(jax.ShapeDtypeStruct((4, half), F32),
                       jax.ShapeDtypeStruct((1, 128), F32),
                       jax.ShapeDtypeStruct((tok, dim), BF16),
                       jax.ShapeDtypeStruct((rows, dim), F32),
                       jax.ShapeDtypeStruct((dim, dim), F32),
                       jax.ShapeDtypeStruct((4, dim), F32)),
            in_specs=[vmem] * 7,
            out_specs=(vmem, vmem, vmem, pl.BlockSpec(memory_space=pl.ANY), vmem, vmem),
            scratch_shapes=[
                pltpu.VMEM((n, tok, dim), BF16),
                pltpu.VMEM((2, n, tok, dim), BF16),
                pltpu.VMEM((dim, rows), BF16),
                pltpu.VMEM((rows, dim), F32),
                pltpu.VMEM((rows, 2 * tok), BF16),
                pltpu.VMEM((n, 8, half), F32),
                pltpu.VMEM((n, 8, half), F32),
                pltpu.VMEM((n, 8, half), F32),
                pltpu.VMEM((8, half), F32),
                pltpu.VMEM((n, 8, half), F32),
                pltpu.VMEM((2, 2, 2, dim + 8, half), F32),
                pltpu.VMEM((n, 2, dim + 8, half), F32),
                pltpu.VMEM((n, 2, dim + 8, half), F32),
                pltpu.VMEM((2, dim, tok), F32),
                pltpu.VMEM((n, width, tok), BF16),
                pltpu.VMEM((n, width, tok), BF16),
                pltpu.VMEM((n, width, dim), F32),
                pltpu.VMEM((8, dim), F32),
                pltpu.VMEM((n, 8, dim), F32),
                pltpu.VMEM((2 * tok, dim), BF16),
                dma((3, n // 2, 2)), dma((n, 2)),
                dma((n,)), dma((n,)), dma((n,)), dma((n,)), dma((n,)), dma((n,)),
                dma((n,)), dma((n,)), dma((n, 2)), dma((n, 2)),
                dma((n,)), dma((n,)), dma((n,)), dma((n,)), dma((n,)), dma((n,)),
                dma,
            ],
            compiler_params=pltpu.CompilerParams(collective_id=0, has_side_effects=True,
                                                 vmem_limit_bytes=67043328),
        )(hidden, w_two, ln_scale, ln_shift, ln_scale.T, embed, meta)
        loss, total, d_hidden, d_embed, d_w_two, d_ln = outs
        return (loss.reshape(2, tok), total[0, :1], d_hidden, d_embed, d_w_two, d_ln[0:2], d_ln[2:4])

    return jax.shard_map(device_step, mesh=mesh,
                         in_specs=(tok_spec, P(), P(), P(), P('tp', None), row_spec, row_spec),
                         out_specs=(row_spec, P('dp'), tok_spec, tok_spec, P('dp', None), P('dp', None), P('dp', None)),
                         check_vma=False)
```

```python
import functools

import jax
import jax.numpy as jnp
from jax import lax
from jax.experimental import pallas as pl
from jax.experimental.pallas import tpu as pltpu
from jax.sharding import PartitionSpec as P

LN_EPS = 1e-5
F32 = jnp.float32
BF16 = jnp.bfloat16
MESH = pl.DeviceIdType.MESH
MASKED = 3.0e38
GROUP = 64


def dot_nn(a, b):
    return lax.dot_general(a, b, (((1,), (0,)), ((), ())), preferred_element_type=F32)


def dot_nt(a, b):
    return lax.dot_general(a, b, (((1,), (1,)), ((), ())), preferred_element_type=F32)


def norm_rows(val, gain, bias):
    cen = val - jnp.mean(val, axis=-1, keepdims=True)
    var = jnp.mean(cen * cen, axis=-1, keepdims=True)
    return (cen * lax.rsqrt(var + LN_EPS) * gain + bias).astype(BF16)


def kernel(n, chunk, h_ref, w_ref, gain_ref, bias_ref, e_ref, tgt_ref, mask_ref,
           loss_ref, total_ref, dh_ref, de_out, dw_ref, dsc_ref, dsh_ref,
           h_all, x_all, et, de, dz, meta_own, meta_all, st_loc, st_rcv, nm_own, nm_all, lse_own, gcol,
           part, sib, ring, at_own, g_own, g_rcv, dwt, sm_own, sm_rcv, xu,
           h_ss, h_rs, meta_ss, meta_rs, st_ss, st_rs, nm_ss, nm_rs, sib_ss, sib_rs, ring_ss, ring_rs,
           g_ss, g_rs, dwt_ss, dwt_rs, sm_ss, sm_rs, de_sem):
    tok, dim = h_ref.shape
    half = tok // 2
    rows = e_ref.shape[0]
    chips = n // 2
    far = chips // 2
    units = n
    width = dim // n
    cols = dim // half
    me = lax.axis_index('tp')
    zc = me // 2
    kc = lax.rem(me, 2)
    wrap = lambda c: lax.rem(c + 2 * chips, chips)
    right = wrap(zc + 1) * 2 + kc
    left = wrap(zc - 1) * 2 + kc
    other = zc * 2 + 1 - kc
    peer = lambda i: lax.rem(me + i, n)

    def rcopy(src, dst, ss, rs, dev):
        return pltpu.make_async_remote_copy(src_ref=src, dst_ref=dst, send_sem=ss, recv_sem=rs,
                                            device_id={'tp': dev}, device_id_type=MESH)

    def each(lo, hi, fn):
        def go(i, c):
            fn(i)
            return c
        lax.fori_loop(lo, hi, go, 0)

    tgt_f = tgt_ref[...].astype(F32)
    mask_f = mask_ref[...].astype(F32)
    meta_own[...] = jnp.concatenate([v[h:h + 1, p * half:(p + 1) * half]
                                     for v in (tgt_f, mask_f) for h in range(2) for p in range(2)], axis=0)

    barrier = pltpu.get_barrier_semaphore()
    each(1, n, lambda i: pl.semaphore_signal(barrier, inc=1, device_id={'tp': peer(i)}, device_id_type=MESH))
    pl.semaphore_wait(barrier, n - 1)

    def gcopy(g, kind, chip, p, core, src=None):
        buf, ss, rs = g
        owner = chip * 2 + core
        cut = buf.shape[1] // 2
        rng = pl.ds(p * cut, cut)
        at = buf.at[owner, rng]
        return rcopy(at if src is None else src.at[rng], at, ss.at[kind, chip, p], rs.at[owner, p],
                     (right, left, other)[kind])

    own_order = ((0, 0), (1, 1), (2, 0), (2, 1), (0, 1), (1, 0))

    def gather_own(g, src=None):
        for kind, p in own_order:
            gcopy(g, kind, zc, p, kc, src).start()

    def gather_step(g, j):
        lo = wrap(zc - j)
        hi = wrap(zc + j)

        @pl.when(j < far)
        def _():
            for p in range(2):
                gcopy(g, 0, lo, p, kc).wait_recv()
                if p == 0:
                    gcopy(g, 0, lo, p, kc).start()
                else:
                    @pl.when(j < far - 1)
                    def _():
                        gcopy(g, 0, lo, p, kc).start()
                gcopy(g, 2, lo, p, kc).start()
                q = 1 - p
                gcopy(g, 1, hi, q, kc).wait_recv()
                if q == 1:
                    gcopy(g, 1, hi, q, kc).start()
                else:
                    @pl.when(j < far - 1)
                    def _():
                        gcopy(g, 1, hi, q, kc).start()
                gcopy(g, 2, hi, q, kc).start()

        @pl.when(j == far)
        def _():
            for p in range(2):
                gcopy(g, p, lo, p, kc).wait_recv()
                gcopy(g, 2, lo, p, kc).start()

    def gather_other(g, chip):
        for p in range(2):
            gcopy(g, 2, chip, p, 1 - kc).wait_recv()

    def gather_done(g, src=None):
        for kind, p in own_order:
            gcopy(g, kind, zc, p, kc, src).wait_send()

        def sent(j):
            lo = wrap(zc - j)
            hi = wrap(zc + j)
            gcopy(g, 0, lo, 0, kc).wait_send()
            gcopy(g, 1, hi, 1, kc).wait_send()

            @pl.when(j < far - 1)
            def _():
                gcopy(g, 0, lo, 1, kc).wait_send()
                gcopy(g, 1, hi, 0, kc).wait_send()
            for p in range(2):
                gcopy(g, 2, lo, p, kc).wait_send()
                gcopy(g, 2, hi, p, kc).wait_send()
        each(1, far, sent)
        for p in range(2):
            gcopy(g, 2, wrap(zc + far), p, kc).wait_send()

    h_net = (h_all, h_ss, h_rs)
    dw_net = (dwt, dwt_ss, dwt_rs)
    gather_own(h_net, h_ref)

    def bcast(src, dst, ss, rs):
        each(1, n, lambda i: rcopy(src, dst.at[me], ss.at[peer(i)], rs.at[me], peer(i)).start())

    def wait_recv(dst, ss, rs):
        each(1, n, lambda i: rcopy(dst.at[peer(i)], dst.at[peer(i)], ss.at[peer(i)], rs.at[peer(i)],
                                   peer(i)).wait_recv())

    def wait_send(dst, ss, rs):
        each(1, n, lambda i: rcopy(dst.at[peer(i)], dst.at[peer(i)], ss.at[peer(i)], rs.at[peer(i)],
                                   peer(i)).wait_send())

    bcast(meta_own, meta_all, meta_ss, meta_rs)
    meta_all[me] = meta_own[...]
    h_all[me] = h_ref[...]

    r_i = lax.broadcasted_iota(jnp.int32, (dim, dim), 0)
    c_i = lax.broadcasted_iota(jnp.int32, (dim, dim), 1)
    eye = jnp.where(r_i == c_i, 1.0, 0.0).astype(BF16)
    for r0 in range(0, rows, chunk):
        et[:, r0:r0 + chunk] = dot_nt(eye, e_ref[r0:r0 + chunk, :]).astype(BF16)
    h_own = h_ref[...]
    at_own[0] = dot_nt(eye, h_own)
    at_own[1] = dot_nt(eye, dot_nn(h_own, w_ref[...]).astype(BF16))
    for h in range(2):
        gcol[h] = jnp.broadcast_to(gain_ref[h:h + 1, :], (half, dim)).T

    def normalize(chip):
        w_two = w_ref[...]
        x_two = []
        for q in range(2):
            a_two = dot_nn(h_all[2 * chip + q], w_two).astype(BF16).astype(F32)
            x_two.append(norm_rows(a_two, gain_ref[1:2, :], bias_ref[1:2, :]))
        for q in range(2):
            x_all[1, 2 * chip + q] = x_two[q]
            x_all[0, 2 * chip + q] = norm_rows(h_all[2 * chip + q].astype(F32), gain_ref[0:1, :], bias_ref[0:1, :])
        return jnp.concatenate(x_two, axis=0)

    def stored(h, chip):
        return x_all[h, pl.ds(2 * chip, 2)].reshape(2 * tok, dim)

    def first_pass(jobs):
        stream = [(k, r0) for k in range(len(jobs)) for r0 in range(0, rows, chunk)]
        logits = lambda k, r0: dot_nt(e_ref[r0:r0 + chunk, :], jobs[k][2])
        z = logits(*stream[0])
        m = s = None
        for at, (k, r0) in enumerate(stream):
            z_next = logits(*stream[at + 1]) if at + 1 < len(stream) else None
            for g in range(0, chunk, GROUP):
                z3 = z[g:g + GROUP, :].reshape(GROUP // 8, 8, 2 * tok)
                cm = jnp.max(z3, axis=0)
                if r0 + g == 0:
                    m = cm
                    s = jnp.sum(jnp.exp(z3 - m[None]), axis=0)
                else:
                    mn = jnp.maximum(m, cm)
                    s = s * jnp.exp(m - mn) + jnp.sum(jnp.exp(z3 - mn[None]), axis=0)
                    m = mn
            if r0 + chunk == rows:
                h, chip, _ = jobs[k]
                m_all = jnp.max(m, axis=0, keepdims=True)
                s_all = jnp.sum(s * jnp.exp(m - m_all), axis=0, keepdims=True)
                for q in range(2):
                    for p in range(2):
                        cut = slice((2 * q + p) * half, (2 * q + p + 1) * half)
                        st_loc[h, 2 * chip + q, p:p + 1, :] = m_all[:, cut]
                        st_loc[h, 2 * chip + q, 2 + p:3 + p, :] = s_all[:, cut]
            z = z_next
        for h, chip, _ in jobs:
            for q in range(2):
                o = 2 * chip + q

                @pl.when(o != me)
                def _():
                    rcopy(st_loc.at[h, o], st_rcv.at[h, me], st_ss.at[h, o], st_rs.at[h, me], o).start()

    def head_count(h):
        two = jnp.sum(jnp.sum(meta_all[:, 4 + 2 * h:6 + 2 * h, :], axis=0), axis=1, keepdims=True)
        return jnp.sum(two, axis=0, keepdims=True)

    def combine(h):
        st_rcv[h, me] = st_loc[h, me]
        wait_recv(st_rcv.at[h], st_ss.at[h], st_rs.at[h])
        mask = meta_own[4 + 2 * h:6 + 2 * h, :]
        weight = mask / head_count(h)
        st = st_rcv[h]
        st_m, st_s = st[:, 0:2, :], st[:, 2:4, :]
        m_tok = jnp.max(st_m, axis=0)
        s_tok = jnp.sum(st_s * jnp.exp(st_m - m_tok[None]), axis=0)
        lse = m_tok + jnp.log(s_tok)
        lse_w = jnp.where(mask > 0.0, lse - jnp.log(jnp.maximum(weight, 1e-30)), MASKED)
        lse_own[h, 0:2, :] = lse
        nm_own[h] = jnp.concatenate([lse_w, weight, jnp.zeros((4, half), F32)], axis=0)
        nm_all[h, me] = nm_own[h]
        bcast(nm_own.at[h], nm_all.at[h], nm_ss.at[h], nm_rs.at[h])

    def stage(k):
        lo = wrap(zc - k)
        hi = wrap(zc + k)
        one = jnp.where(k == 0, zc, wrap(zc + far))

        @pl.when(k == 0)
        def _():
            gather_other(h_net, zc)

        @pl.when((k > 0) & (k <= far))
        def _():
            gather_step(h_net, k)

        @pl.when((k > 0) & (k < far))
        def _():
            gather_other(h_net, lo)
            gather_other(h_net, hi)
            first_pass([(1, lo, normalize(lo)), (1, hi, normalize(hi))])

        @pl.when(k == far)
        def _():
            gather_other(h_net, one)

        @pl.when((k == 0) | (k == far))
        def _():
            first_pass([(1, one, normalize(one))])

        @pl.when((k > 0) & (k <= far) & (k != far - 1))
        def _():
            back = jnp.minimum(k, far - 1)
            near = (wrap(zc - back), wrap(zc + back))
            first_pass([(0, c, stored(0, c)) for c in near])

        @pl.when(k == far + 1)
        def _():
            wait_recv(meta_all, meta_ss, meta_rs)
            combine(1)

        @pl.when((k == 0) | (k == far + 1))
        def _():
            first_pass([(0, one, stored(0, one))])
    each(0, far + 2, stage)
    de[...] = jnp.zeros_like(de)
    wait_recv(nm_all.at[1], nm_ss.at[1], nm_rs.at[1])

    sub_i = lax.broadcasted_iota(jnp.int32, (8, half), 0)
    base_row = (me * rows).astype(F32)

    def pick(tile, row):
        return jnp.sum(jnp.where(sub_i == row, tile, 0.0), axis=0, keepdims=True)

    def sib_copy(u):
        return rcopy(part.at[lax.rem(u, 2), 1 - kc], sib.at[u], sib_ss.at[u], sib_rs.at[u], other)

    cuts = ((0, dim // 2), (dim // 2, dim // 2 + 8))

    def ring_copy(u, d, ab):
        rng = pl.ds(*cuts[ab])
        return rcopy(sib.at[u, d, rng], ring.at[u, d, rng], ring_ss.at[u, d, ab], ring_rs.at[u, d, ab],
                     (right, left)[d])

    def pass_on(u, ab):
        step = lax.rem(u, chips)
        rng = pl.ds(*cuts[ab])
        slot = lax.rem(u, 2)
        if ab == 0:
            sib_copy(u).wait_recv()
        for d in range(2):
            @pl.when(step > 0)
            def _():
                ring_copy(u - 1, d, ab).wait_recv()
                sib[u, d, rng] = sib[u, d, rng] + part[slot, kc, d, rng] + ring[u - 1, d, rng]

            @pl.when(step == 0)
            def _():
                sib[u, d, rng] = sib[u, d, rng] + part[slot, kc, d, rng]

            @pl.when(step < chips - 1)
            def _():
                ring_copy(u, d, ab).start()

    def finish(h, u):
        acc_s = acc_b = None
        da_h, frac = [], []
        n_tok = head_count(h)
        for p in range(2):
            a = at_own[h, :, p * half:(p + 1) * half]
            cen = a - jnp.mean(a, axis=0, keepdims=True)
            rstd = lax.rsqrt(jnp.mean(cen * cen, axis=0, keepdims=True) + LN_EPS)
            xh = cen * rstd
            dx = sib[u, p, 0:dim, :]
            tgt = jnp.sum(sib[u, p, dim:dim + 8, :], axis=0, keepdims=True)
            row = (lse_own[h, p:p + 1, :] - tgt) * meta_own[4 + 2 * h + p:5 + 2 * h + p, :]
            loss_ref[h:h + 1, p * half:(p + 1) * half] = row
            frac.append(row / n_tok)
            dy = dx * gcol[h]
            c1 = jnp.mean(dy, axis=0, keepdims=True)
            c2 = jnp.mean(dy * xh, axis=0, keepdims=True)
            da_h.append(rstd * (dy - c1 - xh * c2))
            acc_s = dx * xh if acc_s is None else acc_s + dx * xh
            acc_b = dx if acc_b is None else acc_b + dx
        d_sc = jnp.sum(acc_s.T, axis=0, keepdims=True)
        d_sh = jnp.sum(acc_b.T, axis=0, keepdims=True)
        lines = [v[:, j * half:(j + 1) * half] for v in (d_sc, d_sh) for j in range(cols)] + frac
        sm_own[h] = jnp.concatenate(lines + [jnp.zeros((16 - len(lines), half), F32)], axis=0)
        sm_rcv[h, me] = sm_own[h]
        bcast(sm_own.at[h], sm_rcv.at[h], sm_ss.at[h], sm_rs.at[h])
        return jnp.concatenate(da_h, axis=1)

    def events(u):
        @pl.when(u == 1)
        def _():
            combine(0)

        @pl.when(u == 5)
        def _():
            wait_recv(nm_all.at[0], nm_ss.at[0], nm_rs.at[0])

        @pl.when(u == chips)
        def _():
            d_proj = finish(1, chips - 1).astype(BF16)
            for i in range(n):
                g_own[i] = d_proj[i * width:(i + 1) * width, :]
            g_rcv[me] = g_own[me]
            each(1, n, lambda i: rcopy(g_own.at[peer(i)], g_rcv.at[me], g_ss.at[peer(i)], g_rs.at[me],
                                       peer(i)).start())
            at_own[1] = dot_nn(w_ref[...], d_proj)

        @pl.when(u == chips + 2)
        def _():
            wait_recv(g_rcv, g_ss, g_rs)
            dw_slice = jnp.zeros((width, dim), F32)
            for o in range(n):
                dw_slice = dw_slice + dot_nn(g_rcv[o], h_all[o])
            dwt[me] = dw_slice
            gather_own(dw_net)

        @pl.when((u > chips + 2) & (u <= chips + 2 + far))
        def _():
            gather_step(dw_net, u - chips - 2)

        @pl.when(u == units - 1)
        def _():
            each(0, chips, lambda c: gather_other(dw_net, c))
            dw_ref[...] = dwt[...].reshape(dim, dim).T

    def unit(u):
        h = 1 - u // chips
        step = lax.rem(u, chips)
        plus = wrap(zc - 1 - step)
        minus = wrap(zc + 1 + step)
        lse_p, w_p, t_p = [], [], []
        for q in range(2):
            for p, chip in ((0, plus), (1, minus)):
                o = 2 * chip + q
                at = 2 * q + p
                xu[at * half:(at + 1) * half, :] = x_all[h, o, p * half:(p + 1) * half, :]
                tile = nm_all[h, o]
                lse_p.append(tile[p:p + 1, :])
                w_p.append(tile[2 + p:3 + p, :])
                t_p.append(pick(meta_all[o], 2 * h + p))
        lse_v = jnp.broadcast_to(jnp.concatenate(lse_p, axis=1), (8, 2 * tok))
        w_v = jnp.broadcast_to(jnp.concatenate(w_p, axis=1), (8, 2 * tok))
        row8 = lax.broadcasted_iota(jnp.int32, (8, 2 * tok), 0).astype(F32)
        t_v = jnp.broadcast_to(jnp.concatenate(t_p, axis=1), (8, 2 * tok)) - base_row - row8
        x = xu[...]
        tz = jnp.zeros((8, 2 * tok), F32)
        z = dot_nt(e_ref[0:chunk, :], x)
        mid = max(rows - 2 * chunk, 0)
        for r0 in range(0, rows, chunk):
            z_next = dot_nt(e_ref[r0 + chunk:r0 + 2 * chunk, :], x) if r0 + chunk < rows else None
            for g in range(0, chunk, 16):
                pieces = []
                for b in range(2):
                    z8 = z[g + 8 * b:g + 8 * b + 8, :]
                    hit = t_v == float(r0 + g + 8 * b)
                    tz = tz + jnp.where(hit, z8, 0.0)
                    pieces.append(jnp.exp(z8 - lse_v) - jnp.where(hit, w_v, 0.0))
                dz[r0 + g:r0 + g + 16, :] = jnp.concatenate(pieces, axis=0).astype(BF16)
            de[r0:r0 + chunk, :] += dot_nn(dz[r0:r0 + chunk, :], x)
            z = z_next
            if r0 == mid:
                @pl.when(u >= 1)
                def _():
                    pass_on(u - 1, 0)
        dxt = dot_nn(et[...], dz[...])

        @pl.when(u >= 2)
        def _():
            sib_copy(u - 2).wait_send()
        slot = lax.rem(u, 2)
        for q in range(2):
            for p in range(2):
                cut = slice((2 * q + p) * half, (2 * q + p + 1) * half)
                part[slot, q, p, 0:dim, :] = dxt[:, cut]
                part[slot, q, p, dim:dim + 8, :] = tz[:, cut]
        sib_copy(u).start()

        @pl.when(u >= 1)
        def _():
            pass_on(u - 1, 1)
        events(u)
    each(0, units, unit)
    de_copy = pltpu.make_async_copy(de, de_out, de_sem)
    de_copy.start()
    last = units - 1
    pass_on(last, 0)
    pass_on(last, 1)
    d_a1 = finish(0, last)
    dh_ref[...] = (d_a1 + at_own[1]).T.astype(BF16)

    wait_send(meta_all, meta_ss, meta_rs)
    for h in range(2):
        wait_send(st_rcv.at[h], st_ss.at[h], st_rs.at[h])
        wait_send(nm_all.at[h], nm_ss.at[h], nm_rs.at[h])
        wait_send(sm_rcv.at[h], sm_ss.at[h], sm_rs.at[h])
    wait_send(g_rcv, g_ss, g_rs)
    gather_done(h_net, h_ref)
    gather_done(dw_net)
    for u in (units - 2, units - 1):
        sib_copy(u).wait_send()

    def ring_done(u):
        @pl.when(lax.rem(u, chips) < chips - 1)
        def _():
            for d in range(2):
                for ab in range(2):
                    ring_copy(u, d, ab).wait_send()
    each(0, units, ring_done)

    for h in (1, 0):
        wait_recv(sm_rcv.at[h], sm_ss.at[h], sm_rs.at[h])
    total = 0.0
    for h in range(2):
        sm = jnp.sum(sm_rcv[h], axis=0)
        for j in range(cols):
            dsc_ref[h:h + 1, j * half:(j + 1) * half] = sm[j:j + 1, :]
            dsh_ref[h:h + 1, j * half:(j + 1) * half] = sm[cols + j:cols + j + 1, :]
        total = total + jnp.sum(sm[2 * cols:2 * cols + 2, :])
    total_ref[0] = total
    de_copy.wait()


def pick_chunk(rows):
    best = 128
    for c in range(128, min(rows, 640) + 1, 128):
        if rows % c == 0:
            best = c
    return best


def solution(mesh):
    n = mesh.shape['tp']
    tok_spec = P(('dp', 'tp'), None)
    row_spec = P(None, ('dp', 'tp'))

    def device_step(hidden, w_two, ln_scale, ln_shift, embed, targets, loss_mask):
        tok, dim = hidden.shape
        half = tok // 2
        rows = embed.shape[0]
        width = dim // n
        vmem = pl.BlockSpec(memory_space=pltpu.VMEM)
        dma = pltpu.SemaphoreType.DMA
        return pl.pallas_call(
            functools.partial(kernel, n, pick_chunk(rows)),
            name='two_head_step',
            out_shape=(jax.ShapeDtypeStruct((2, tok), F32),
                       jax.ShapeDtypeStruct((1,), F32),
                       jax.ShapeDtypeStruct((tok, dim), BF16),
                       jax.ShapeDtypeStruct((rows, dim), F32),
                       jax.ShapeDtypeStruct((dim, dim), F32),
                       jax.ShapeDtypeStruct((2, dim), F32),
                       jax.ShapeDtypeStruct((2, dim), F32)),
            in_specs=[vmem] * 7,
            out_specs=(vmem, pl.BlockSpec(memory_space=pltpu.SMEM), vmem, pl.BlockSpec(memory_space=pl.ANY),
                       vmem, vmem, vmem),
            scratch_shapes=[
                pltpu.VMEM((n, tok, dim), BF16),
                pltpu.VMEM((2, n, tok, dim), BF16),
                pltpu.VMEM((dim, rows), BF16),
                pltpu.VMEM((rows, dim), F32),
                pltpu.VMEM((rows, 2 * tok), BF16),
                pltpu.VMEM((8, half), F32),
                pltpu.VMEM((n, 8, half), F32),
                pltpu.VMEM((2, n, 8, half), F32),
                pltpu.VMEM((2, n, 8, half), F32),
                pltpu.VMEM((2, 8, half), F32),
                pltpu.VMEM((2, n, 8, half), F32),
                pltpu.VMEM((2, 8, half), F32),
                pltpu.VMEM((2, dim, half), F32),
                pltpu.VMEM((2, 2, 2, dim + 8, half), F32),
                pltpu.VMEM((n, 2, dim + 8, half), F32),
                pltpu.VMEM((n, 2, dim + 8, half), F32),
                pltpu.VMEM((2, dim, tok), F32),
                pltpu.VMEM((n, width, tok), BF16),
                pltpu.VMEM((n, width, tok), BF16),
                pltpu.VMEM((n, width, dim), F32),
                pltpu.VMEM((2, 16, half), F32),
                pltpu.VMEM((2, n, 16, half), F32),
                pltpu.VMEM((2 * tok, dim), BF16),
                dma((3, n // 2, 2)), dma((n, 2)),
                dma((n,)), dma((n,)), dma((2, n)), dma((2, n)), dma((2, n)), dma((2, n)),
                dma((n,)), dma((n,)), dma((n, 2, 2)), dma((n, 2, 2)),
                dma((n,)), dma((n,)), dma((3, n // 2, 2)), dma((n, 2)), dma((2, n)), dma((2, n)),
                dma,
            ],
            compiler_params=pltpu.CompilerParams(collective_id=0, has_side_effects=True,
                                                 vmem_limit_bytes=67043328),
        )(hidden, w_two, ln_scale, ln_shift, embed, targets, loss_mask)

    return jax.shard_map(device_step, mesh=mesh,
                         in_specs=(tok_spec, P(), P(), P(), P('tp', None), row_spec, row_spec),
                         out_specs=(row_spec, P('dp'), tok_spec, tok_spec, P('dp', None), P('dp', None), P('dp', None)),
                         check_vma=False)
```

```python
import functools

import jax
import jax.numpy as jnp
from jax import lax
from jax.experimental import pallas as pl
from jax.experimental.pallas import tpu as pltpu
from jax.sharding import PartitionSpec as P

LN_EPS = 1e-5
F32 = jnp.float32
BF16 = jnp.bfloat16
MESH = pl.DeviceIdType.MESH
MASKED = 3.0e38
GROUP = 64


def dot_nn(a, b):
    return lax.dot_general(a, b, (((1,), (0,)), ((), ())), preferred_element_type=F32)


def dot_nt(a, b):
    return lax.dot_general(a, b, (((1,), (1,)), ((), ())), preferred_element_type=F32)


def norm_rows(val, gain, bias):
    cen = val - jnp.mean(val, axis=-1, keepdims=True)
    var = jnp.mean(cen * cen, axis=-1, keepdims=True)
    return (cen * lax.rsqrt(var + LN_EPS) * gain + bias).astype(BF16)


def kernel(n, chunk, h_ref, w_ref, gain_ref, bias_ref, e_ref, tgt_ref, mask_ref,
           loss_ref, total_ref, dh_ref, de_out, dw_ref, dsc_ref, dsh_ref,
           h_all, x_all, et, de, dz, meta_own, meta_all, st_loc, st_rcv, nm_own, nm_all, lse_own, gcol,
           part, sib, ring, at_own, g_own, g_rcv, dwt, sm_own, sm_rcv, xu,
           h_ss, h_rs, meta_ss, meta_rs, st_ss, st_rs, nm_ss, nm_rs, sib_ss, sib_rs, ring_ss, ring_rs,
           g_ss, g_rs, dwt_ss, dwt_rs, sm_ss, sm_rs, de_sem):
    tok, dim = h_ref.shape
    half = tok // 2
    rows = e_ref.shape[0]
    chips = n // 2
    far = chips // 2
    units = n
    width = dim // n
    cols = dim // half
    me = lax.axis_index('tp')
    zc = me // 2
    kc = lax.rem(me, 2)
    wrap = lambda c: lax.rem(c + 2 * chips, chips)
    right = wrap(zc + 1) * 2 + kc
    left = wrap(zc - 1) * 2 + kc
    other = zc * 2 + 1 - kc
    peer = lambda i: lax.rem(me + i, n)

    def rcopy(src, dst, ss, rs, dev):
        return pltpu.make_async_remote_copy(src_ref=src, dst_ref=dst, send_sem=ss, recv_sem=rs,
                                            device_id={'tp': dev}, device_id_type=MESH)

    def each(lo, hi, fn):
        def go(i, c):
            fn(i)
            return c
        lax.fori_loop(lo, hi, go, 0)

    tgt_f = tgt_ref[...].astype(F32)
    mask_f = mask_ref[...].astype(F32)
    meta_own[...] = jnp.concatenate([v[h:h + 1, p * half:(p + 1) * half]
                                     for v in (tgt_f, mask_f) for h in range(2) for p in range(2)], axis=0)

    barrier = pltpu.get_barrier_semaphore()
    each(1, n, lambda i: pl.semaphore_signal(barrier, inc=1, device_id={'tp': peer(i)}, device_id_type=MESH))
    pl.semaphore_wait(barrier, n - 1)

    def gcopy(g, kind, chip, p, core, src=None):
        buf, ss, rs = g
        owner = chip * 2 + core
        cut = buf.shape[1] // 2
        rng = pl.ds(p * cut, cut)
        at = buf.at[owner, rng]
        return rcopy(at if src is None else src.at[rng], at, ss.at[kind, chip, p], rs.at[owner, p],
                     (right, left, other)[kind])

    own_order = ((0, 0), (1, 1), (2, 0), (2, 1), (0, 1), (1, 0))

    def gather_own(g, src=None):
        for kind, p in own_order:
            gcopy(g, kind, zc, p, kc, src).start()

    def gather_step(g, j):
        lo = wrap(zc - j)
        hi = wrap(zc + j)

        @pl.when(j < far)
        def _():
            for p in range(2):
                gcopy(g, 0, lo, p, kc).wait_recv()
                if p == 0:
                    gcopy(g, 0, lo, p, kc).start()
                else:
                    @pl.when(j < far - 1)
                    def _():
                        gcopy(g, 0, lo, p, kc).start()
                gcopy(g, 2, lo, p, kc).start()
                q = 1 - p
                gcopy(g, 1, hi, q, kc).wait_recv()
                if q == 1:
                    gcopy(g, 1, hi, q, kc).start()
                else:
                    @pl.when(j < far - 1)
                    def _():
                        gcopy(g, 1, hi, q, kc).start()
                gcopy(g, 2, hi, q, kc).start()

        @pl.when(j == far)
        def _():
            for p in range(2):
                gcopy(g, p, lo, p, kc).wait_recv()
                gcopy(g, 2, lo, p, kc).start()

    def gather_other(g, chip):
        for p in range(2):
            gcopy(g, 2, chip, p, 1 - kc).wait_recv()

    def gather_done(g, src=None):
        for kind, p in own_order:
            gcopy(g, kind, zc, p, kc, src).wait_send()

        def sent(j):
            lo = wrap(zc - j)
            hi = wrap(zc + j)
            gcopy(g, 0, lo, 0, kc).wait_send()
            gcopy(g, 1, hi, 1, kc).wait_send()

            @pl.when(j < far - 1)
            def _():
                gcopy(g, 0, lo, 1, kc).wait_send()
                gcopy(g, 1, hi, 0, kc).wait_send()
            for p in range(2):
                gcopy(g, 2, lo, p, kc).wait_send()
                gcopy(g, 2, hi, p, kc).wait_send()
        each(1, far, sent)
        for p in range(2):
            gcopy(g, 2, wrap(zc + far), p, kc).wait_send()

    h_net = (h_all, h_ss, h_rs)
    dw_net = (dwt, dwt_ss, dwt_rs)
    gather_own(h_net, h_ref)

    def bcast(src, dst, ss, rs):
        each(1, n, lambda i: rcopy(src, dst.at[me], ss.at[peer(i)], rs.at[me], peer(i)).start())

    def wait_recv(dst, ss, rs):
        each(1, n, lambda i: rcopy(dst.at[peer(i)], dst.at[peer(i)], ss.at[peer(i)], rs.at[peer(i)],
                                   peer(i)).wait_recv())

    def wait_send(dst, ss, rs):
        each(1, n, lambda i: rcopy(dst.at[peer(i)], dst.at[peer(i)], ss.at[peer(i)], rs.at[peer(i)],
                                   peer(i)).wait_send())

    bcast(meta_own, meta_all, meta_ss, meta_rs)
    meta_all[me] = meta_own[...]
    h_all[me] = h_ref[...]

    r_i = lax.broadcasted_iota(jnp.int32, (dim, dim), 0)
    c_i = lax.broadcasted_iota(jnp.int32, (dim, dim), 1)
    eye = jnp.where(r_i == c_i, 1.0, 0.0).astype(BF16)
    for r0 in range(0, rows, chunk):
        et[:, r0:r0 + chunk] = dot_nt(eye, e_ref[r0:r0 + chunk, :]).astype(BF16)
    h_own = h_ref[...]
    at_own[0] = dot_nt(eye, h_own)
    at_own[1] = dot_nt(eye, dot_nn(h_own, w_ref[...]).astype(BF16))
    for h in range(2):
        gcol[h] = jnp.broadcast_to(gain_ref[h:h + 1, :], (half, dim)).T

    def normalize(chip):
        w_two = w_ref[...]
        x_two = []
        for q in range(2):
            a_two = dot_nn(h_all[2 * chip + q], w_two).astype(BF16).astype(F32)
            x_two.append(norm_rows(a_two, gain_ref[1:2, :], bias_ref[1:2, :]))
        for q in range(2):
            x_all[1, 2 * chip + q] = x_two[q]
            x_all[0, 2 * chip + q] = norm_rows(h_all[2 * chip + q].astype(F32), gain_ref[0:1, :], bias_ref[0:1, :])
        return jnp.concatenate(x_two, axis=0)

    def stored(h, chip):
        return x_all[h, pl.ds(2 * chip, 2)].reshape(2 * tok, dim)

    def first_pass(jobs):
        stream = [(k, r0) for k in range(len(jobs)) for r0 in range(0, rows, chunk)]
        logits = lambda k, r0: dot_nt(e_ref[r0:r0 + chunk, :], jobs[k][2])
        z = logits(*stream[0])
        m = s = None
        for at, (k, r0) in enumerate(stream):
            z_next = logits(*stream[at + 1]) if at + 1 < len(stream) else None
            for g in range(0, chunk, GROUP):
                z3 = z[g:g + GROUP, :].reshape(GROUP // 8, 8, 2 * tok)
                cm = jnp.max(z3, axis=0)
                if r0 + g == 0:
                    m = cm
                    s = jnp.sum(jnp.exp(z3 - m[None]), axis=0)
                else:
                    mn = jnp.maximum(m, cm)
                    s = s * jnp.exp(m - mn) + jnp.sum(jnp.exp(z3 - mn[None]), axis=0)
                    m = mn
            if r0 + chunk == rows:
                h, chip, _ = jobs[k]
                m_all = jnp.max(m, axis=0, keepdims=True)
                s_all = jnp.sum(s * jnp.exp(m - m_all), axis=0, keepdims=True)
                for q in range(2):
                    for p in range(2):
                        cut = slice((2 * q + p) * half, (2 * q + p + 1) * half)
                        st_loc[h, 2 * chip + q, p:p + 1, :] = m_all[:, cut]
                        st_loc[h, 2 * chip + q, 2 + p:3 + p, :] = s_all[:, cut]
            z = z_next
        for h, chip, _ in jobs:
            for q in range(2):
                o = 2 * chip + q

                @pl.when(o != me)
                def _():
                    rcopy(st_loc.at[h, o], st_rcv.at[h, me], st_ss.at[h, o], st_rs.at[h, me], o).start()

    def head_count(h):
        two = jnp.sum(jnp.sum(meta_all[:, 4 + 2 * h:6 + 2 * h, :], axis=0), axis=1, keepdims=True)
        return jnp.sum(two, axis=0, keepdims=True)

    def combine(h):
        st_rcv[h, me] = st_loc[h, me]
        wait_recv(st_rcv.at[h], st_ss.at[h], st_rs.at[h])
        mask = meta_own[4 + 2 * h:6 + 2 * h, :]
        weight = mask / head_count(h)
        st = st_rcv[h]
        st_m, st_s = st[:, 0:2, :], st[:, 2:4, :]
        m_tok = jnp.max(st_m, axis=0)
        s_tok = jnp.sum(st_s * jnp.exp(st_m - m_tok[None]), axis=0)
        lse = m_tok + jnp.log(s_tok)
        lse_w = jnp.where(mask > 0.0, lse - jnp.log(jnp.maximum(weight, 1e-30)), MASKED)
        lse_own[h, 0:2, :] = lse
        nm_own[h] = jnp.concatenate([lse_w, weight, jnp.zeros((4, half), F32)], axis=0)
        nm_all[h, me] = nm_own[h]
        bcast(nm_own.at[h], nm_all.at[h], nm_ss.at[h], nm_rs.at[h])

    def stage(k):
        lo = wrap(zc - k)
        hi = wrap(zc + k)
        one = jnp.where(k == 0, zc, wrap(zc + far))

        @pl.when(k == 0)
        def _():
            gather_other(h_net, zc)

        @pl.when((k > 0) & (k <= far))
        def _():
            gather_step(h_net, k)

        @pl.when((k > 0) & (k < far))
        def _():
            gather_other(h_net, lo)
            gather_other(h_net, hi)
            first_pass([(1, lo, normalize(lo)), (1, hi, normalize(hi))])

        @pl.when(k == far)
        def _():
            gather_other(h_net, one)

        @pl.when((k == 0) | (k == far))
        def _():
            first_pass([(1, one, normalize(one))])

        @pl.when((k > 0) & (k <= far) & (k != far - 1))
        def _():
            back = jnp.minimum(k, far - 1)
            near = (wrap(zc - back), wrap(zc + back))
            first_pass([(0, c, stored(0, c)) for c in near])

        @pl.when(k == far + 1)
        def _():
            wait_recv(meta_all, meta_ss, meta_rs)
            combine(1)

        @pl.when((k == 0) | (k == far + 1))
        def _():
            first_pass([(0, one, stored(0, one))])
    each(0, far + 2, stage)
    de[...] = jnp.zeros_like(de)
    wait_recv(nm_all.at[1], nm_ss.at[1], nm_rs.at[1])

    sub_i = lax.broadcasted_iota(jnp.int32, (8, half), 0)
    base_row = (me * rows).astype(F32)

    def pick(tile, row):
        return jnp.sum(jnp.where(sub_i == row, tile, 0.0), axis=0, keepdims=True)

    def sib_copy(u):
        return rcopy(part.at[lax.rem(u, 2), 1 - kc], sib.at[u], sib_ss.at[u], sib_rs.at[u], other)

    cuts = ((0, dim // 2), (dim // 2, dim // 2 + 8))

    def ring_copy(u, d, ab):
        rng = pl.ds(*cuts[ab])
        return rcopy(sib.at[u, d, rng], ring.at[u, d, rng], ring_ss.at[u, d, ab], ring_rs.at[u, d, ab],
                     (right, left)[d])

    def pass_on(u, ab):
        step = lax.rem(u, chips)
        rng = pl.ds(*cuts[ab])
        slot = lax.rem(u, 2)
        if ab == 0:
            sib_copy(u).wait_recv()
        for d in range(2):
            @pl.when(step > 0)
            def _():
                ring_copy(u - 1, d, ab).wait_recv()
                sib[u, d, rng] = sib[u, d, rng] + part[slot, kc, d, rng] + ring[u - 1, d, rng]

            @pl.when(step == 0)
            def _():
                sib[u, d, rng] = sib[u, d, rng] + part[slot, kc, d, rng]

            @pl.when(step < chips - 1)
            def _():
                ring_copy(u, d, ab).start()

    def finish(h, u):
        acc_s = acc_b = None
        da_h, frac = [], []
        n_tok = head_count(h)
        for p in range(2):
            a = at_own[h, :, p * half:(p + 1) * half]
            cen = a - jnp.mean(a, axis=0, keepdims=True)
            rstd = lax.rsqrt(jnp.mean(cen * cen, axis=0, keepdims=True) + LN_EPS)
            xh = cen * rstd
            dx = sib[u, p, 0:dim, :]
            tgt = jnp.sum(sib[u, p, dim:dim + 8, :], axis=0, keepdims=True)
            row = (lse_own[h, p:p + 1, :] - tgt) * meta_own[4 + 2 * h + p:5 + 2 * h + p, :]
            loss_ref[h:h + 1, p * half:(p + 1) * half] = row
            frac.append(row / n_tok)
            dy = dx * gcol[h]
            c1 = jnp.mean(dy, axis=0, keepdims=True)
            c2 = jnp.mean(dy * xh, axis=0, keepdims=True)
            da_h.append(rstd * (dy - c1 - xh * c2))
            acc_s = dx * xh if acc_s is None else acc_s + dx * xh
            acc_b = dx if acc_b is None else acc_b + dx
        d_sc = jnp.sum(acc_s.T, axis=0, keepdims=True)
        d_sh = jnp.sum(acc_b.T, axis=0, keepdims=True)
        lines = [v[:, j * half:(j + 1) * half] for v in (d_sc, d_sh) for j in range(cols)] + frac
        sm_own[h] = jnp.concatenate(lines + [jnp.zeros((16 - len(lines), half), F32)], axis=0)
        sm_rcv[h, me] = sm_own[h]
        bcast(sm_own.at[h], sm_rcv.at[h], sm_ss.at[h], sm_rs.at[h])
        return jnp.concatenate(da_h, axis=1)

    def events(u):
        @pl.when(u == 1)
        def _():
            combine(0)

        @pl.when(u == 5)
        def _():
            wait_recv(nm_all.at[0], nm_ss.at[0], nm_rs.at[0])

        @pl.when(u == chips)
        def _():
            d_proj = finish(1, chips - 1).astype(BF16)
            for i in range(n):
                g_own[i] = d_proj[i * width:(i + 1) * width, :]
            g_rcv[me] = g_own[me]
            each(1, n, lambda i: rcopy(g_own.at[peer(i)], g_rcv.at[me], g_ss.at[peer(i)], g_rs.at[me],
                                       peer(i)).start())
            at_own[1] = dot_nn(w_ref[...], d_proj)

        @pl.when(u == chips + 2)
        def _():
            wait_recv(g_rcv, g_ss, g_rs)
            dw_slice = jnp.zeros((width, dim), F32)
            for o in range(n):
                dw_slice = dw_slice + dot_nn(g_rcv[o], h_all[o])
            dwt[me] = dw_slice
            gather_own(dw_net)

        @pl.when((u > chips + 2) & (u <= chips + 2 + far))
        def _():
            gather_step(dw_net, u - chips - 2)

        @pl.when(u == units - 1)
        def _():
            each(0, chips, lambda c: gather_other(dw_net, c))
            dw_ref[...] = dwt[...].reshape(dim, dim).T

    def unit(u):
        h = 1 - u // chips
        step = lax.rem(u, chips)
        plus = wrap(zc - 1 - step)
        minus = wrap(zc + 1 + step)
        lse_p, w_p, t_p = [], [], []
        for q in range(2):
            for p, chip in ((0, plus), (1, minus)):
                o = 2 * chip + q
                at = 2 * q + p
                xu[at * half:(at + 1) * half, :] = x_all[h, o, p * half:(p + 1) * half, :]
                tile = nm_all[h, o]
                lse_p.append(tile[p:p + 1, :])
                w_p.append(tile[2 + p:3 + p, :])
                t_p.append(pick(meta_all[o], 2 * h + p))
        lse_v = jnp.broadcast_to(jnp.concatenate(lse_p, axis=1), (8, 2 * tok))
        w_v = jnp.broadcast_to(jnp.concatenate(w_p, axis=1), (8, 2 * tok))
        row8 = lax.broadcasted_iota(jnp.int32, (8, 2 * tok), 0).astype(F32)
        t_v = jnp.broadcast_to(jnp.concatenate(t_p, axis=1), (8, 2 * tok)) - base_row - row8
        x = xu[...]
        tz = jnp.zeros((8, 2 * tok), F32)
        z = dot_nt(e_ref[0:chunk, :], x)
        mid = max(rows - 2 * chunk, 0)
        for r0 in range(0, rows, chunk):
            z_next = dot_nt(e_ref[r0 + chunk:r0 + 2 * chunk, :], x) if r0 + chunk < rows else None
            for g in range(0, chunk, 16):
                pieces = []
                for b in range(2):
                    z8 = z[g + 8 * b:g + 8 * b + 8, :]
                    hit = t_v == float(r0 + g + 8 * b)
                    tz = tz + jnp.where(hit, z8, 0.0)
                    pieces.append(jnp.exp(z8 - lse_v) - jnp.where(hit, w_v, 0.0))
                dz[r0 + g:r0 + g + 16, :] = jnp.concatenate(pieces, axis=0).astype(BF16)
            de[r0:r0 + chunk, :] += dot_nn(dz[r0:r0 + chunk, :], x)
            z = z_next
            if r0 == mid:
                @pl.when(u >= 1)
                def _():
                    pass_on(u - 1, 0)
        dxt = dot_nn(et[...], dz[...])

        @pl.when(u >= 2)
        def _():
            sib_copy(u - 2).wait_send()
        slot = lax.rem(u, 2)
        for q in range(2):
            for p in range(2):
                cut = slice((2 * q + p) * half, (2 * q + p + 1) * half)
                part[slot, q, p, 0:dim, :] = dxt[:, cut]
                part[slot, q, p, dim:dim + 8, :] = tz[:, cut]
        sib_copy(u).start()

        @pl.when(u >= 1)
        def _():
            pass_on(u - 1, 1)
        events(u)
    each(0, units, unit)
    de_copy = pltpu.make_async_copy(de, de_out, de_sem)
    de_copy.start()
    last = units - 1
    pass_on(last, 0)
    pass_on(last, 1)
    d_a1 = finish(0, last)
    dh_ref[...] = (d_a1 + at_own[1]).T.astype(BF16)

    wait_send(meta_all, meta_ss, meta_rs)
    for h in range(2):
        wait_send(st_rcv.at[h], st_ss.at[h], st_rs.at[h])
        wait_send(nm_all.at[h], nm_ss.at[h], nm_rs.at[h])
        wait_send(sm_rcv.at[h], sm_ss.at[h], sm_rs.at[h])
    wait_send(g_rcv, g_ss, g_rs)
    gather_done(h_net, h_ref)
    gather_done(dw_net)
    for u in (units - 2, units - 1):
        sib_copy(u).wait_send()

    def ring_done(u):
        @pl.when(lax.rem(u, chips) < chips - 1)
        def _():
            for d in range(2):
                for ab in range(2):
                    ring_copy(u, d, ab).wait_send()
    each(0, units, ring_done)

    for h in (1, 0):
        wait_recv(sm_rcv.at[h], sm_ss.at[h], sm_rs.at[h])
    total = 0.0
    for h in range(2):
        sm = jnp.sum(sm_rcv[h], axis=0)
        for j in range(cols):
            dsc_ref[h:h + 1, j * half:(j + 1) * half] = sm[j:j + 1, :]
            dsh_ref[h:h + 1, j * half:(j + 1) * half] = sm[cols + j:cols + j + 1, :]
        total = total + jnp.sum(sm[2 * cols:2 * cols + 2, :])
    total_ref[0] = total
    de_copy.wait()


def pick_chunk(rows):
    best = 128
    for c in range(128, min(rows, 640) + 1, 128):
        if rows % c == 0:
            best = c
    return best


def flush_kernel(*refs):
    count = len(refs) // 2

    @pl.when(pl.program_id(0) == 0)
    def _():
        refs[count][0] = refs[0][0]
        for i in range(2, count):
            refs[count + i][...] = refs[i][...]
    refs[count + 1][...] = refs[1][...]


def flush(total, d_embed, *small):
    rows, dim = d_embed.shape
    block = pick_chunk(rows)
    big = pl.BlockSpec((block, dim), lambda i: (i, 0))
    specs = [pl.BlockSpec(memory_space=pltpu.SMEM), big] + [pl.BlockSpec(v.shape, lambda i: (0, 0)) for v in small]
    outs = [total, d_embed, *small]
    return pl.pallas_call(flush_kernel, name='flush', grid=(rows // block,), in_specs=specs, out_specs=specs,
                          out_shape=[jax.ShapeDtypeStruct(v.shape, v.dtype) for v in outs])(*outs)


def solution(mesh):
    n = mesh.shape['tp']
    tok_spec = P(('dp', 'tp'), None)
    row_spec = P(None, ('dp', 'tp'))

    def device_step(hidden, w_two, ln_scale, ln_shift, embed, targets, loss_mask):
        tok, dim = hidden.shape
        half = tok // 2
        rows = embed.shape[0]
        width = dim // n
        vmem = pl.BlockSpec(memory_space=pltpu.VMEM)
        dma = pltpu.SemaphoreType.DMA
        loss, total, d_hidden, d_embed, d_w_two, d_sc, d_sh, *_ = pl.pallas_call(
            functools.partial(kernel, n, pick_chunk(rows)),
            name='two_head_step',
            out_shape=(jax.ShapeDtypeStruct((2, tok), F32),
                       jax.ShapeDtypeStruct((1,), F32),
                       jax.ShapeDtypeStruct((tok, dim), BF16),
                       jax.ShapeDtypeStruct((rows, dim), F32),
                       jax.ShapeDtypeStruct((dim, dim), F32),
                       jax.ShapeDtypeStruct((2, dim), F32),
                       jax.ShapeDtypeStruct((2, dim), F32)),
            in_specs=[vmem] * 7,
            out_specs=(vmem, pl.BlockSpec(memory_space=pltpu.SMEM), vmem, pl.BlockSpec(memory_space=pl.ANY),
                       vmem, vmem, vmem),
            scratch_shapes=[
                pltpu.VMEM((n, tok, dim), BF16),
                pltpu.VMEM((2, n, tok, dim), BF16),
                pltpu.VMEM((dim, rows), BF16),
                pltpu.VMEM((rows, dim), F32),
                pltpu.VMEM((rows, 2 * tok), BF16),
                pltpu.VMEM((8, half), F32),
                pltpu.VMEM((n, 8, half), F32),
                pltpu.VMEM((2, n, 8, half), F32),
                pltpu.VMEM((2, n, 8, half), F32),
                pltpu.VMEM((2, 8, half), F32),
                pltpu.VMEM((2, n, 8, half), F32),
                pltpu.VMEM((2, 8, half), F32),
                pltpu.VMEM((2, dim, half), F32),
                pltpu.VMEM((2, 2, 2, dim + 8, half), F32),
                pltpu.VMEM((n, 2, dim + 8, half), F32),
                pltpu.VMEM((n, 2, dim + 8, half), F32),
                pltpu.VMEM((2, dim, tok), F32),
                pltpu.VMEM((n, width, tok), BF16),
                pltpu.VMEM((n, width, tok), BF16),
                pltpu.VMEM((n, width, dim), F32),
                pltpu.VMEM((2, 16, half), F32),
                pltpu.VMEM((2, n, 16, half), F32),
                pltpu.VMEM((2 * tok, dim), BF16),
                dma((3, n // 2, 2)), dma((n, 2)),
                dma((n,)), dma((n,)), dma((2, n)), dma((2, n)), dma((2, n)), dma((2, n)),
                dma((n,)), dma((n,)), dma((n, 2, 2)), dma((n, 2, 2)),
                dma((n,)), dma((n,)), dma((3, n // 2, 2)), dma((n, 2)), dma((2, n)), dma((2, n)),
                dma,
            ],
            compiler_params=pltpu.CompilerParams(collective_id=0, has_side_effects=True,
                                                 vmem_limit_bytes=67043328),
        )(hidden, w_two, ln_scale, ln_shift, embed, targets, loss_mask)
        total, d_embed, loss, d_hidden, d_w_two, d_sc, d_sh = flush(total, d_embed, loss, d_hidden, d_w_two, d_sc, d_sh)
        return loss, total, d_hidden, d_embed, d_w_two, d_sc, d_sh

    return jax.shard_map(device_step, mesh=mesh,
                         in_specs=(tok_spec, P(), P(), P(), P('tp', None), row_spec, row_spec),
                         out_specs=(row_spec, P('dp'), tok_spec, tok_spec, P('dp', None), P('dp', None), P('dp', None)),
                         check_vma=False)
```
